32 devices in a mesh: groups: 2 (over y), ctx: 8 (over z, x), head: 2 (over core).
Axes of the slice: x: 2, y: 2, z: 4, core: 2. Of those that a mesh axis runs over, the one named last changes fastest.
Arguments:
- queries: bfloat16 [16, 128, 64, 192], P(('groups', 'ctx'), None, 'head'), parts along dimension 0, may hold values from -360 to 360
- latent_pages: bfloat16 [16, 8, 64, 576], P(('groups', 'ctx'), 'head'), parts along dimension 0, may hold values from -6 to 6
- page_scales: bfloat16 [16, 8, 4, 64], P(('groups', 'ctx'), 'head'), parts along dimension 0, may hold values from 0.5 to 2
- page_table: int32 [16, 8], P(('groups', 'ctx')), parts along dimension 0, may hold values from 0 to 7, each once within a row
- lengths: int32 [16], P(('groups', 'ctx')), parts along dimension 0, may hold values from 128 to 512, as said below
- w_keys: bfloat16 [512, 64, 128], P('ctx', 'head'), may hold values from -0.5 to 0.5
- w_values: bfloat16 [512, 64, 128], P('ctx', 'head'), may hold values from -1 to 1
Outputs:
- attended: bfloat16 [16, 128, 64, 128], P(('groups', 'ctx'), None, 'head'), parts along dimension 0
The draws below stay inside these ranges and needn't reach their ends.
There are 2 independent parts, one for each index of `groups`. The reference program is written for one: setup_inputs(seed, part) draws one part's arguments, and reference() takes and returns one part's arrays. A program takes and returns all parts, laid end to end along the dimension named above; an argument that names none is the same for every part. Nothing has to cross between parts.
Inputs may be any that keep to these rules, and one draw needn't show every extreme that they name: `page_table`: each row is a permutation of 0 to 7. `lengths`: a length counts the cached tokens and the 128 rows of the span, which take the last positions; the longest request of a part has exactly 512 tokens.
All inputs are finite; a program needn't handle non-finite values.
Results may differ from the reference program's by a relative error of at most 0.0084.
Values may be sent and summed in bfloat16 or wider, within the bound.
No kernel may reach another device: no remote copies, remote signals or barrier semaphores. Data moves between devices by JAX's collectives and lax.ppermute only.
A program may use at most 64 MiB of HBM per device.

```python
import math
import jax
import jax.numpy as jnp
from jax import lax

HEADS = 64
NOPE = 128
ROPE = 64
VDIM = 128
LATENT = 512
GROUPS = 4
PAGE = 64
SPAN = 128
PAGES_REQ = 8
REQS = 8


def draw_latent_pages(key, part):
    code_key = jax.random.fold_in(key, 202)
    rope_key = jax.random.fold_in(key, 303)
    code_values = jnp.clip(jax.random.normal(code_key, (REQS, PAGES_REQ, PAGE, LATENT), jnp.float32), -6.0, 6.0)
    rotary = jnp.clip(jax.random.normal(rope_key, (REQS, PAGES_REQ, PAGE, ROPE), jnp.float32), -4.0, 4.0)
    return jnp.concatenate([code_values, rotary], axis=-1).astype(jnp.bfloat16)


def draw_queries(key, part):
    full_shape = (REQS, SPAN, HEADS, NOPE + ROPE)
    main_key = jax.random.fold_in(key, 404)
    drawn = jnp.clip(jax.random.normal(main_key, full_shape, jnp.float32), -6.0, 6.0)
    return drawn.astype(jnp.bfloat16)


def draw_lengths(key, part):
    longest_tokens = PAGES_REQ * PAGE
    reach = longest_tokens - SPAN + 1
    first_key = jax.random.fold_in(key, 606)
    second_key = jax.random.fold_in(key, 707)
    third_key = jax.random.fold_in(key, 808)
    first_draw = jax.random.randint(first_key, (REQS,), 0, reach, jnp.int32)
    second_draw = jax.random.randint(second_key, (REQS,), 0, reach, jnp.int32)
    extra_tokens = first_draw * second_draw // reach
    chosen_request = jax.random.randint(third_key, (), 0, REQS, jnp.int32)
    result = SPAN + extra_tokens
    return result.at[chosen_request].set(longest_tokens)


def steps_of(stream_key, dims, shards, least, top_value):
    loudness, own = 1.0, jax.random.fold_in(stream_key, 6)
    for axis_at, parts in shards:
        draws = jnp.exp(jax.random.uniform(jax.random.fold_in(own, axis_at), (parts,), jnp.float32, least / len(shards), top_value / len(shards)))
        loudness = loudness * jnp.repeat(draws, dims[axis_at] // parts).reshape([-1 if axis == axis_at else 1 for axis in range(len(dims))])
    return loudness


def gaussian(rng, extent, width, limit, cuts=(), dtype=jnp.bfloat16):
    array = width * jax.random.normal(rng, extent, jnp.float32)
    if cuts:
        array = array * steps_of(rng, extent, cuts, -0.22, 0.18)
    return jnp.clip(array, -limit, limit).astype(dtype)


def setup_inputs(seed: int = 0, part: int = 0) -> dict:
    seeds = jax.random.split(jax.random.key(seed), 8)
    own_keys = jax.random.split(jax.random.fold_in(seeds[7], part), 8)
    queries = draw_queries(jax.random.fold_in(jax.random.fold_in(seeds[7], part), 71), part)
    latent_pages = draw_latent_pages(jax.random.fold_in(jax.random.fold_in(seeds[7], part), 71), part)
    page_scales = jnp.clip(jnp.exp(math.log(2.0) - 1.3862944 * jax.random.uniform(own_keys[2], (REQS, PAGES_REQ, GROUPS, PAGE), jnp.float32) ** steps_of(own_keys[2], (REQS, PAGES_REQ, GROUPS, PAGE), ((0, 8), (1, 2)), -0.2, 0.2)), 0.5, 2.0).astype(jnp.bfloat16)
    page_table = jax.vmap(lambda own: jax.random.permutation(own, PAGES_REQ))(jax.random.split(own_keys[3], REQS)).reshape((REQS, PAGES_REQ)).astype(jnp.int32)
    lengths = draw_lengths(jax.random.fold_in(jax.random.fold_in(seeds[7], part), 71), part)
    w_keys = gaussian(seeds[5], (LATENT, HEADS, NOPE), (LATENT // 4) ** -0.5, 0.5, ((0, 8), (1, 2)))
    w_values = gaussian(seeds[6], (LATENT, HEADS, VDIM), (LATENT // 16) ** -0.5, 1.0, ((0, 8), (1, 2)))
    return {"queries": queries, "latent_pages": latent_pages, "page_scales": page_scales, "page_table": page_table, "lengths": lengths, "w_keys": w_keys, "w_values": w_values}


def one_request(span_query, pool_pages, pool_scales, pool_table, length_one, w_keys, w_values):
    ordered = jnp.take(pool_pages, pool_table.astype(jnp.int32), axis=0)
    ordered_scales = jnp.take(pool_scales, pool_table.astype(jnp.int32), axis=0)
    key_count = PAGES_REQ * PAGE
    code_values = ordered[:, :, :LATENT].astype(jnp.float32).reshape(PAGES_REQ, PAGE, GROUPS, LATENT // GROUPS)
    factor = jnp.swapaxes(ordered_scales, 1, 2).astype(jnp.float32)[..., None]
    latent = (code_values * factor).reshape(key_count, LATENT).astype(jnp.bfloat16)
    rotary = ordered[:, :, LATENT:].reshape(key_count, ROPE)
    key_nope = jnp.dot(latent, w_keys.reshape(LATENT, HEADS * NOPE), preferred_element_type=jnp.float32)
    key_nope = key_nope.astype(jnp.bfloat16).reshape(key_count, HEADS, NOPE)
    value_rows = jnp.dot(latent, w_values.reshape(LATENT, HEADS * VDIM), preferred_element_type=jnp.float32)
    value_rows = value_rows.astype(jnp.bfloat16).reshape(key_count, HEADS, VDIM)
    query_nope = span_query[:, :, :NOPE].astype(jnp.float32)
    query_rope = span_query[:, :, NOPE:].astype(jnp.float32)
    scores = jnp.einsum('chn,khn->hck', query_nope, key_nope.astype(jnp.float32))
    scores = scores + jnp.einsum('chr,kr->hck', query_rope, rotary.astype(jnp.float32))
    scores = scores * (1.0 / math.sqrt(NOPE + ROPE))
    row_position = lax.broadcasted_iota(jnp.int32, (SPAN, key_count), 0)
    key_position = lax.broadcasted_iota(jnp.int32, (SPAN, key_count), 1)
    visible = (key_position <= length_one.astype(jnp.int32) - SPAN + row_position)[None]
    row_top = lax.optimization_barrier(jnp.max(jnp.where(visible, scores, -jnp.inf), axis=2))
    raw_weight = jnp.where(visible, jnp.exp(scores - row_top[..., None]), 0.0)
    row_total = lax.optimization_barrier(jnp.sum(raw_weight, axis=2))
    weights = raw_weight.astype(jnp.bfloat16)
    summed = jnp.einsum('hck,khv->chv', weights.astype(jnp.float32), value_rows.astype(jnp.float32))
    return (summed / jnp.swapaxes(row_total, 0, 1)[..., None]).astype(jnp.bfloat16)

def reference(queries, latent_pages, page_scales, page_table, lengths, w_keys, w_values):

    def handle(operands):
        return one_request(operands[0], operands[1], operands[2], operands[3], operands[4], w_keys, w_values)
    return lax.map(handle, (queries, latent_pages, page_scales, page_table, lengths))
```

```python
import functools
import math

import jax
import jax.numpy as jnp
from jax import lax
from jax.experimental import pallas as pl
from jax.experimental.pallas import tpu as pltpu
from jax.sharding import PartitionSpec as P

NEGATIVE = -1e30
LANES = 128
CHUNKS = 2


def packed_weights(position, w_keys, w_values, share):
    rows, _, key_width = w_keys.shape
    value_width = w_values.shape[2]
    per = share // CHUNKS
    widths = (key_width, value_width)

    def kernel(position_ref, keys_ref, values_ref, *rest):
        outs, wide = rest[:CHUNKS], rest[CHUNKS:]
        for ref, flat in zip((keys_ref, values_ref), wide):
            flat[...] = ref[...].astype(jnp.float32).reshape(flat.shape)
        for chunk in range(CHUNKS):
            start = 0
            for flat, width in zip(wide, widths):
                for head in range(per):
                    one = flat[pl.ds(chunk * per + head, rows, stride=share), :]
                    outs[chunk][:, pl.ds(start, width)] = one.astype(jnp.bfloat16)
                    start += width

    return pl.pallas_call(
        kernel,
        grid_spec=pltpu.PrefetchScalarGridSpec(
            num_scalar_prefetch=1,
            grid=(1,),
            in_specs=[
                pl.BlockSpec((rows, share, width), lambda i, where: (0, where[0], 0))
                for width in widths
            ],
            out_specs=[
                pl.BlockSpec((rows, per * sum(widths)), lambda i, where: (0, 0))
                for _ in range(CHUNKS)
            ],
            scratch_shapes=[pltpu.VMEM((rows * share, width), jnp.float32) for width in widths],
        ),
        out_shape=[jax.ShapeDtypeStruct((rows, per * sum(widths)), jnp.bfloat16)] * CHUNKS,
        cost_estimate=pl.CostEstimate(
            flops=10_000_000, bytes_accessed=4 * rows * share * sum(widths), transcendentals=0
        ),
        name="packed_weights",
    )(position, w_keys, w_values)


def packed_latents(position, pages, scales, table, length, row_count):
    page_count, page_rows, width = pages.shape
    groups = scales.shape[1]
    slots = table.shape[1]
    latent = width - width % LANES
    rotary = width - latent
    group_width = latent // groups

    def kernel(position_ref, pages_ref, scales_ref, table_ref, length_ref, out_ref):
        group_of = lax.broadcasted_iota(jnp.int32, (groups, latent), 1) // group_width
        row_of = lax.broadcasted_iota(jnp.int32, (groups, latent), 0)
        spread = jnp.where(group_of == row_of, 1.0, 0.0).astype(jnp.bfloat16)
        first = length_ref[0] - row_count
        for page in range(page_count):
            factor = lax.dot_general(
                scales_ref[page], spread, (((0,), (0,)), ((), ())),
                preferred_element_type=jnp.float32,
            )
            here = pl.ds(page * page_rows, page_rows)
            codes = pages_ref[page, :, :latent].astype(jnp.float32)
            out_ref[here, :latent] = (codes * factor).astype(jnp.bfloat16)
            slot = position_ref[2] * page_count + page
            logical = jnp.int32(0)
            for at in range(slots):
                logical += jnp.where(table_ref[0, at] == slot, at, 0)
            token = lax.broadcasted_iota(jnp.int32, (page_rows, LANES - rotary), 0)
            threshold = jnp.clip(logical * page_rows + token - first, 0, row_count)
            out_ref[here, latent:] = jnp.concatenate(
                [pages_ref[page, :, latent:], threshold.astype(jnp.float32).astype(jnp.bfloat16)],
                axis=1,
            )

    return pl.pallas_call(
        kernel,
        in_specs=[
            pl.BlockSpec(memory_space=pltpu.SMEM),
            pl.BlockSpec(memory_space=pltpu.VMEM),
            pl.BlockSpec(memory_space=pltpu.VMEM),
            pl.BlockSpec(memory_space=pltpu.SMEM),
            pl.BlockSpec(memory_space=pltpu.SMEM),
        ],
        out_shape=jax.ShapeDtypeStruct((page_count * page_rows, latent + LANES), jnp.bfloat16),
        cost_estimate=pl.CostEstimate(
            flops=10_000_000, bytes_accessed=4 * page_count * page_rows * width, transcendentals=0
        ),
        name="packed_latents",
    )(position, pages, scales, table, length)


def attend(
    position, tokens, queries, query_share, query_head, pieces, offsets, key_width, per,
    into=None, heads_out=None,
):
    token_rows, token_width = tokens[0].shape
    key_count = token_rows * len(tokens)
    latent = token_width - LANES
    query_width, row_count = queries.shape[1:]
    rotary = query_width - key_width
    chunk_width = pieces[0].shape[1]
    value_width = chunk_width // per - key_width
    piece_rows = pieces[0].shape[0]
    ring = len(pieces)
    scale = 1.0 / math.sqrt(query_width)
    aliased = into is not None
    pair = 2 if per % 2 == 0 else 1

    def kernel(position_ref, *refs):
        token_refs, refs = refs[: len(tokens)], refs[len(tokens) :]
        query_ref, refs = refs[0], refs[1:]
        piece_refs, refs = refs[:ring], refs[ring:]
        if aliased:
            refs = refs[1:]
        out_ref, held, weight, query, bias, result, sem = refs
        copies = []
        for at, ref in enumerate(token_refs):
            copies.append((ref, held.at[pl.ds(at * token_rows, token_rows)]))
        start = query_head + position_ref[0] * query_share
        copies.append((query_ref.at[pl.ds(start, per)], query))
        for ref, offset in zip(piece_refs, offsets):
            if ring == 1:
                row = 0
            else:
                ctx = position_ref[1]
                place = jnp.where(ctx % 2 == 0, ctx // 2, ring - 1 - ctx // 2)
                place = (place + offset + ring) % ring
                ctx = jnp.where(place < ring // 2, 2 * place, 2 * (ring - 1 - place) + 1)
                row = pl.multiple_of(ctx * piece_rows, piece_rows)
            copies.append((ref, weight.at[pl.ds(row, piece_rows)]))
        copies = [pltpu.make_async_copy(a, b, sem.at[i]) for i, (a, b) in enumerate(copies)]
        for copy in copies:
            copy.start()
        for copy in copies:
            copy.wait()
        tail = held[:, latent:].astype(jnp.float32).T
        row_of = lax.broadcasted_iota(jnp.int32, (row_count, key_count), 0)
        visible = tail[rotary : rotary + 1, :] <= row_of.astype(jnp.float32)
        bias[...] = jnp.where(visible, 0.0, NEGATIVE)

        def heads(step, carry):
            at = pl.multiple_of(step * pair * key_width, pair * key_width)
            keys = jnp.dot(
                held[:, :latent], weight[:, pl.ds(at, pair * key_width)],
                preferred_element_type=jnp.float32,
            ).astype(jnp.bfloat16)
            at = pl.multiple_of(step * pair * value_width, LANES)
            values = jnp.dot(
                held[:, :latent],
                weight[:, pl.ds(per * key_width + at, pair * value_width)],
                preferred_element_type=jnp.float32,
            ).astype(jnp.bfloat16)
            for one in range(pair):
                head = step * pair + one
                key = jnp.concatenate(
                    [
                        keys[:, one * key_width : (one + 1) * key_width],
                        held[:, latent : latent + rotary],
                    ],
                    axis=1,
                )
                score = lax.dot_general(
                    query[head].T, key, (((1,), (1,)), ((), ())),
                    preferred_element_type=jnp.float32,
                )
                score = score * scale + bias[...]
                top = jnp.max(score, axis=1, keepdims=True)
                raw = jnp.exp(score - top)
                total = jnp.sum(raw, axis=1, keepdims=True)
                out = jnp.dot(
                    raw.astype(jnp.bfloat16),
                    values[:, one * value_width : (one + 1) * value_width],
                    preferred_element_type=jnp.float32,
                )
                result[pl.ds(head, row_count, stride=per), :] = out / total
            return carry

        lax.fori_loop(0, per // pair, heads, 0)
        out_ref[...] = result[...].reshape(out_ref.shape).astype(jnp.bfloat16)

    flops = 4 * key_count * latent * chunk_width // 2 + 2 * per * row_count * key_count * 384
    operands = [*tokens, queries, *pieces]
    if aliased:
        operands.append(into)
    total_heads = per if heads_out is None else heads_out
    block = query_head // per

    def out_at(i, where):
        return (0, 0 if heads_out is None else where[0] * (query_share // per) + block, 0)

    return pl.pallas_call(
        kernel,
        grid_spec=pltpu.PrefetchScalarGridSpec(
            num_scalar_prefetch=1,
            grid=(1,),
            in_specs=[pl.BlockSpec(memory_space=pl.ANY)] * len(operands),
            out_specs=pl.BlockSpec((row_count, per, value_width), out_at),
            scratch_shapes=[
                pltpu.VMEM((key_count, token_width), jnp.bfloat16),
                pltpu.VMEM((latent, chunk_width), jnp.bfloat16),
                pltpu.VMEM((per, query_width, row_count), jnp.bfloat16),
                pltpu.VMEM((row_count, key_count), jnp.float32),
                pltpu.VMEM((row_count * per, value_width), jnp.float32),
                pltpu.SemaphoreType.DMA((len(tokens) + 1 + ring,)),
            ],
        ),
        out_shape=jax.ShapeDtypeStruct((row_count, total_heads, value_width), jnp.bfloat16),
        input_output_aliases={len(operands): 0} if aliased else {},
        cost_estimate=pl.CostEstimate(
            flops=flops, bytes_accessed=4_000_000, transcendentals=per * row_count * key_count
        ),
        name="attend",
    )(position, *operands)


def shifts(size, by):
    return [(i, (i + by) % size) for i in range(size)]


def gathered_weights(chunks, size):
    rows = chunks[0].shape[0]
    if size % 2 or size > 8 or rows % 16:
        return [([lax.all_gather(c, "ctx", axis=0, tiled=True)], [0]) for c in chunks]
    order = list(range(0, size, 2)) + list(range(size - 1, 0, -2))
    onward = [(order[i], order[(i + 1) % size]) for i in range(size)]
    back = [(b, a) for a, b in onward]
    pieces = [[c] for c in chunks]
    offsets = [[0] for _ in chunks]
    ahead, behind = list(chunks), list(chunks)
    for step in range(1, size // 2 + 1):
        for c in range(len(chunks)):
            if step < size // 2 or c % 2 == 0:
                ahead[c] = lax.ppermute(ahead[c], "ctx", onward)
                pieces[c].append(ahead[c])
                offsets[c].append(-step)
            if step < size // 2 or c % 2 == 1:
                behind[c] = lax.ppermute(behind[c], "ctx", back)
                pieces[c].append(behind[c])
                offsets[c].append(step)
    return list(zip(pieces, offsets))


def on_device(
    group_size, ctx_size, head_size,
    queries, latent_pages, page_scales, page_table, lengths, w_keys, w_values,
):
    group = lax.axis_index("groups")
    position = jnp.stack([group, lax.axis_index("ctx"), lax.axis_index("head")]).astype(jnp.int32)
    row_count, head_count = queries.shape[1:3]
    key_width = w_keys.shape[2]
    value_width = w_values.shape[2]
    share = head_count // group_size
    per = share // CHUNKS
    chunks = packed_weights(position, w_keys, w_values, share)
    weights = gathered_weights(chunks, ctx_size)
    span = jnp.transpose(queries[0], (1, 2, 0))
    mine = packed_latents(
        position, latent_pages[0], page_scales[0], page_table, lengths, row_count
    )

    def all_tokens(part):
        return [part] + [lax.ppermute(part, "head", shifts(head_size, s)) for s in range(1, head_size)]

    arrived = []
    for s in range(1, group_size):
        part = lax.ppermute(mine, "groups", shifts(group_size, s))
        away = lax.rem(group + s, group_size) * share
        asked = lax.dynamic_slice_in_dim(span, away, share, 0)
        asked = lax.ppermute(asked, "groups", shifts(group_size, s))
        arrived.append((part, asked))
    own_tokens = all_tokens(mine)
    arrived = [(all_tokens(part), asked) for part, asked in arrived]

    out = None
    returned = []
    for c in range(CHUNKS):
        pieces, offsets = weights[c]
        for s in range(1, group_size):
            tokens, asked = arrived[s - 1]
            block = attend(
                position, tokens, asked, 0, c * per, pieces, offsets, key_width, per
            )
            block = lax.ppermute(block, "groups", shifts(group_size, -s))
            returned.append((s, c, block))
        out = attend(
            position, own_tokens, span, share, c * per, pieces, offsets, key_width, per,
            into=out, heads_out=head_count,
        )
    for s, c, block in returned:
        first = lax.rem(group + s, group_size) * share + c * per
        out = lax.dynamic_update_slice(out, block, (0, first, 0))
    return out[None]


def solution(mesh):
    return jax.shard_map(
        functools.partial(
            on_device, mesh.shape["groups"], mesh.shape["ctx"], mesh.shape["head"]
        ),
        mesh=mesh,
        in_specs=(
            P(("groups", "ctx"), None, "head", None),
            P(("groups", "ctx"), "head", None, None),
            P(("groups", "ctx"), "head", None, None),
            P(("groups", "ctx"), None),
            P(("groups", "ctx")),
            P("ctx", "head", None),
            P("ctx", "head", None),
        ),
        out_specs=P(("groups", "ctx"), None, "head", None),
        check_vma=False,
    )
```

```python
import functools
import math

import jax
import jax.numpy as jnp
from jax import lax
from jax.experimental import pallas as pl
from jax.experimental.pallas import tpu as pltpu
from jax.sharding import PartitionSpec as P

NEGATIVE = -1e30
LANES = 128
CHUNKS = 2
KERNEL_VMEM = 12 * 1024 * 1024


def ring_place(index, size):
    return jnp.where(index % 2 == 0, index // 2, size - 1 - index // 2)


def ring_index(place, size):
    return jnp.where(place < size // 2, 2 * place, 2 * (size - 1 - place) + 1)


def packed_weights(position, w_keys, w_values, share):
    rows, _, key_width = w_keys.shape
    value_width = w_values.shape[2]
    per = share // CHUNKS
    widths = (key_width, value_width)

    def kernel(position_ref, keys_ref, values_ref, *rest):
        outs, wide = rest[:CHUNKS], rest[CHUNKS:]
        for ref, flat in zip((keys_ref, values_ref), wide):
            flat[...] = ref[...].astype(jnp.float32).reshape(flat.shape)
        for chunk in range(CHUNKS):
            start = 0
            for flat, width in zip(wide, widths):
                for head in range(per):
                    one = flat[pl.ds(chunk * per + head, rows, stride=share), :]
                    outs[chunk][:, pl.ds(start, width)] = one.astype(jnp.bfloat16)
                    start += width

    return pl.pallas_call(
        kernel,
        grid_spec=pltpu.PrefetchScalarGridSpec(
            num_scalar_prefetch=1,
            grid=(1,),
            in_specs=[
                pl.BlockSpec((rows, share, width), lambda i, where: (0, where[0], 0))
                for width in widths
            ],
            out_specs=[
                pl.BlockSpec((rows, per * sum(widths)), lambda i, where: (0, 0))
                for _ in range(CHUNKS)
            ],
            scratch_shapes=[pltpu.VMEM((rows * share, width), jnp.float32) for width in widths],
        ),
        out_shape=[jax.ShapeDtypeStruct((rows, per * sum(widths)), jnp.bfloat16)] * CHUNKS,
        cost_estimate=pl.CostEstimate(
            flops=10_000_000, bytes_accessed=4 * rows * share * sum(widths), transcendentals=0
        ),
        compiler_params=pltpu.CompilerParams(vmem_limit_bytes=KERNEL_VMEM),
        name="packed_weights",
    )(position, w_keys, w_values)


def packed_latents(position, pages, scales, table, length, row_count, ring):
    page_count, page_rows, width = pages.shape
    groups = scales.shape[1]
    slots = table.shape[1]
    latent = width - width % LANES
    rotary = width - latent
    group_width = latent // groups

    def kernel(position_ref, pages_ref, scales_ref, table_ref, length_ref, out_ref):
        group_of = lax.broadcasted_iota(jnp.int32, (groups, latent), 1) // group_width
        row_of = lax.broadcasted_iota(jnp.int32, (groups, latent), 0)
        spread = jnp.where(group_of == row_of, 1.0, 0.0).astype(jnp.bfloat16)
        first = length_ref[0] - row_count
        if ring:
            rows = latent // ring
            column = lax.broadcasted_iota(jnp.int32, (latent, latent), 1)
            turn = column // rows
            offset = jnp.where(turn % 2 == 1, -((turn + 1) // 2), turn // 2)
            source = ring_index((ring_place(position_ref[1], ring) + offset + ring) % ring, ring)
            source = source * rows + column % rows
            own_row = lax.broadcasted_iota(jnp.int32, (latent, latent), 0)
            order = jnp.where(source == own_row, 1.0, 0.0).astype(jnp.bfloat16)
        for page in range(page_count):
            factor = lax.dot_general(
                scales_ref[page], spread, (((0,), (0,)), ((), ())),
                preferred_element_type=jnp.float32,
            )
            here = pl.ds(page * page_rows, page_rows)
            codes = pages_ref[page, :, :latent].astype(jnp.float32)
            values = (codes * factor).astype(jnp.bfloat16)
            if ring:
                values = jnp.dot(values, order, preferred_element_type=jnp.float32)
            out_ref[here, :latent] = values.astype(jnp.bfloat16)
            slot = position_ref[2] * page_count + page
            logical = jnp.int32(0)
            for at in range(slots):
                logical += jnp.where(table_ref[0, at] == slot, at, 0)
            token = lax.broadcasted_iota(jnp.int32, (page_rows, LANES - rotary), 0)
            threshold = jnp.clip(logical * page_rows + token - first, 0, row_count)
            out_ref[here, latent:] = jnp.concatenate(
                [pages_ref[page, :, latent:], threshold.astype(jnp.float32).astype(jnp.bfloat16)],
                axis=1,
            )

    return pl.pallas_call(
        kernel,
        in_specs=[
            pl.BlockSpec(memory_space=pltpu.SMEM),
            pl.BlockSpec(memory_space=pltpu.VMEM),
            pl.BlockSpec(memory_space=pltpu.VMEM),
            pl.BlockSpec(memory_space=pltpu.SMEM),
            pl.BlockSpec(memory_space=pltpu.SMEM),
        ],
        out_shape=jax.ShapeDtypeStruct((page_count * page_rows, latent + LANES), jnp.bfloat16),
        cost_estimate=pl.CostEstimate(
            flops=10_000_000, bytes_accessed=4 * page_count * page_rows * width, transcendentals=0
        ),
        compiler_params=pltpu.CompilerParams(vmem_limit_bytes=KERNEL_VMEM),
        name="packed_latents",
    )(position, pages, scales, table, length)


def attend(tokens, queries, head, pieces, key_width, per, into=None, position=None):
    token_rows, token_width = tokens[0].shape
    key_count = token_rows * len(tokens)
    latent = token_width - LANES
    query_width, row_count = queries.shape[1:]
    rotary = query_width - key_width
    chunk_width = pieces[0].shape[1]
    value_width = chunk_width // per - key_width
    key_columns = per * key_width
    scale = 1.0 / math.sqrt(query_width)
    pair = 2 if per % 2 == 0 else 1
    inner = per // pair
    whole = pl.BlockSpec(memory_space=pltpu.VMEM)

    def kernel(*refs):
        if into is not None:
            refs = refs[1:]
        token_refs, refs = refs[: len(tokens)], refs[len(tokens) :]
        query_ref, refs = refs[0], refs[1:]
        piece_refs, refs = refs[: len(pieces)], refs[len(pieces) :]
        if into is not None and len(into) > 2:
            refs = refs[1:]
        out_ref, keys, values, bias, result = refs

        def columns(start, size):
            blocks = [ref[:, start : start + size] for ref in piece_refs]
            return blocks[0] if len(blocks) == 1 else jnp.concatenate(blocks, axis=0)

        def held(start, size):
            blocks = [ref[:, start : start + size] for ref in token_refs]
            return blocks[0] if len(blocks) == 1 else jnp.concatenate(blocks, axis=0)

        threshold = held(latent, LANES).astype(jnp.float32)[:, rotary : rotary + 1]
        row_of = lax.broadcasted_iota(jnp.int32, (key_count, row_count), 1)
        bias[...] = jnp.where(threshold <= row_of.astype(jnp.float32), 0.0, NEGATIVE)
        values[...] = lax.dot_general(
            columns(key_columns, per * value_width), held(0, latent), (((0,), (1,)), ((), ())),
            preferred_element_type=jnp.float32,
        ).astype(jnp.bfloat16)

        def expand(step):
            at = step * pair * key_width
            keys[:, at : at + pair * key_width] = jnp.dot(
                held(0, latent), columns(at, pair * key_width),
                preferred_element_type=jnp.float32,
            ).astype(jnp.bfloat16)

        def one_head(at):
            key = jnp.concatenate(
                [keys[:, at * key_width : (at + 1) * key_width], held(latent, rotary)], axis=1
            )
            score = jnp.dot(key, query_ref[head + at], preferred_element_type=jnp.float32)
            score = score * scale + bias[...]
            top = jnp.max(score, axis=0, keepdims=True)
            raw = jnp.exp(score - top)
            total = jnp.sum(raw, axis=0, keepdims=True)
            out = jnp.dot(
                values[at * value_width : (at + 1) * value_width, :], raw.astype(jnp.bfloat16),
                preferred_element_type=jnp.float32,
            )
            result[pl.ds(at, row_count, stride=per), :] = (out / total).T

        expand(0)
        for step in range(inner):
            if step + 1 < inner:
                expand(step + 1)
            for at in range(step * pair, (step + 1) * pair):
                one_head(at)
        out_ref[...] = result[...].reshape(out_ref.shape).astype(jnp.bfloat16)

    operands = [*tokens, queries, *pieces]
    in_specs = [whole] * len(operands)
    scratch = [
        pltpu.VMEM((key_count, key_columns), jnp.bfloat16),
        pltpu.VMEM((per * value_width, key_count), jnp.bfloat16),
        pltpu.VMEM((key_count, row_count), jnp.float32),
        pltpu.VMEM((row_count * per, value_width), jnp.float32),
    ]
    extra = dict(
        compiler_params=pltpu.CompilerParams(vmem_limit_bytes=KERNEL_VMEM),
        cost_estimate=pl.CostEstimate(
            flops=2 * key_count * per * (latent * (key_width + value_width) + row_count * 384),
            bytes_accessed=2_000_000,
            transcendentals=per * row_count * key_count,
        ),
        name="attend",
    )
    block = (row_count, per, value_width)
    if into is None:
        return pl.pallas_call(
            kernel,
            in_specs=in_specs,
            out_specs=whole,
            out_shape=jax.ShapeDtypeStruct(block, jnp.bfloat16),
            scratch_shapes=scratch,
            **extra,
        )(*operands)
    total_heads, share = into[0], into[1]
    aliases = {}
    if len(into) > 2:
        operands.append(into[2])
        in_specs.append(pl.BlockSpec(memory_space=pl.ANY))
        aliases = {len(operands): 0}
    return pl.pallas_call(
        kernel,
        grid_spec=pltpu.PrefetchScalarGridSpec(
            num_scalar_prefetch=1,
            grid=(1,),
            in_specs=in_specs,
            out_specs=pl.BlockSpec(
                block, lambda i, where: (0, where[0] * (share // per) + head // per, 0)
            ),
            scratch_shapes=scratch,
        ),
        out_shape=jax.ShapeDtypeStruct((row_count, total_heads, value_width), jnp.bfloat16),
        input_output_aliases=aliases,
        **extra,
    )(position, *operands)


def shifts(size, by):
    return [(i, (i + by) % size) for i in range(size)]


def rings(size, rows):
    return size % 2 == 0 and size <= 8 and rows % 16 == 0


def gathered_weights(chunks, size):
    if not rings(size, chunks[0].shape[0]):
        return [[lax.all_gather(c, "ctx", axis=0, tiled=True)] for c in chunks]
    order = list(range(0, size, 2)) + list(range(size - 1, 0, -2))
    onward = [(order[i], order[(i + 1) % size]) for i in range(size)]
    back = [(b, a) for a, b in onward]
    pieces = [[c] for c in chunks]
    ahead, behind = list(chunks), list(chunks)
    for step in range(1, size // 2 + 1):
        for c in range(len(chunks)):
            if step < size // 2 or c % 2 == 0:
                ahead[c] = lax.ppermute(ahead[c], "ctx", onward)
                pieces[c].append(ahead[c])
            if step < size // 2 or c % 2 == 1:
                behind[c] = lax.ppermute(behind[c], "ctx", back)
                pieces[c].append(behind[c])
    return pieces


def on_device(
    group_size, ctx_size, head_size,
    queries, latent_pages, page_scales, page_table, lengths, w_keys, w_values,
):
    group = lax.axis_index("groups")
    position = jnp.stack([group, lax.axis_index("ctx"), lax.axis_index("head")]).astype(jnp.int32)
    row_count, head_count = queries.shape[1:3]
    key_width = w_keys.shape[2]
    value_width = w_values.shape[2]
    share = head_count // group_size
    per = share // CHUNKS
    chunks = packed_weights(position, w_keys, w_values, share)
    weights = gathered_weights(chunks, ctx_size)
    span = jnp.transpose(queries[0], (1, 2, 0))
    mine = packed_latents(
        position, latent_pages[0], page_scales[0], page_table, lengths, row_count,
        ctx_size if rings(ctx_size, w_keys.shape[0]) else 0,
    )

    def all_tokens(part):
        return [part] + [lax.ppermute(part, "head", shifts(head_size, s)) for s in range(1, head_size)]

    arrived = []
    for s in range(1, group_size):
        part = lax.ppermute(mine, "groups", shifts(group_size, s))
        away = lax.rem(group + s, group_size) * share
        asked = lax.dynamic_slice_in_dim(span, away, share, 0)
        asked = lax.ppermute(asked, "groups", shifts(group_size, s))
        arrived.append((part, asked))
    own_tokens = all_tokens(mine)
    arrived = [(all_tokens(part), asked) for part, asked in arrived]

    own_queries = lax.dynamic_slice_in_dim(span, group * share, share, 0)
    into = (head_count, share)
    returned = []
    for c in range(CHUNKS):
        for s in range(1, group_size):
            tokens, asked = arrived[s - 1]
            block = attend(tokens, asked, c * per, weights[c], key_width, per)
            block = lax.ppermute(block, "groups", shifts(group_size, -s))
            returned.append((s, c, block))
        out = attend(
            own_tokens, own_queries, c * per, weights[c], key_width, per, into, position
        )
        into = (head_count, share, out)
    for s, c, block in returned:
        first = lax.rem(group + s, group_size) * share + c * per
        out = lax.dynamic_update_slice(out, block, (0, first, 0))
    return out[None]


def solution(mesh):
    return jax.shard_map(
        functools.partial(
            on_device, mesh.shape["groups"], mesh.shape["ctx"], mesh.shape["head"]
        ),
        mesh=mesh,
        in_specs=(
            P(("groups", "ctx"), None, "head", None),
            P(("groups", "ctx"), "head", None, None),
            P(("groups", "ctx"), "head", None, None),
            P(("groups", "ctx"), None),
            P(("groups", "ctx")),
            P("ctx", "head", None),
            P("ctx", "head", None),
        ),
        out_specs=P(("groups", "ctx"), None, "head", None),
        check_vma=False,
    )
```
